32 devices in a mesh: af: 4 (over y, x), sa: 8 (over z, core).
Axes of the slice: x: 2, y: 2, z: 4, core: 2. Of those that a mesh axis runs over, the one named last changes fastest.
Arguments:
- data_real: bfloat16 [64, 512, 512], P('af', 'sa'), may hold values from -0.5 to 0.5
- data_imaginary: bfloat16 [64, 512, 512], P('af', 'sa'), may hold values from -0.5 to 0.5
- wavelet_real: float32 [64], P('af'), may hold values from -2.5 to 2.5
- wavelet_imaginary: float32 [64], P('af'), may hold values from -2.5 to 2.5
- primaries_real: float32 [64, 512, 512], P('af', 'sa'), may hold values from -3 to 3
- primaries_imaginary: float32 [64, 512, 512], P('af', 'sa'), may hold values from -3 to 3
Outputs:
- updated_real: float32 [64, 512, 512], P('af', 'sa')
- updated_imaginary: float32 [64, 512, 512], P('af', 'sa')
- misfit: float32 [2], replicated
The draws below stay inside these ranges and needn't reach their ends.
All inputs are finite; a program needn't handle non-finite values.
Results may differ from the reference program's by a relative error of at most 0.0018.
Values may be sent and summed in bfloat16 or wider, within the bound.
A program may use at most 128 MiB of HBM per device.

```python
import jax
import jax.numpy as jnp
from jax import lax

N = 512
F = 64
ITERS = 2


def levels(own_key, dims, cuts, low, top_value):
    gain, own = 1.0, jax.random.fold_in(own_key, 6)
    for axis_at, parts in cuts:
        steps = jnp.exp(jax.random.uniform(jax.random.fold_in(own, axis_at), (parts,), jnp.float32, low / len(cuts), top_value / len(cuts)))
        gain = gain * jnp.repeat(steps, dims[axis_at] // parts).reshape([-1 if axis == axis_at else 1 for axis in range(len(dims))])
    return gain


def scatter_about(rng, shape, deviation, most, pieces=(), kind=jnp.bfloat16):
    gain = levels(rng, shape, pieces, -0.22, 0.18) if pieces else 1.0
    result = jax.random.normal(rng, shape, jnp.float32) * deviation * gain
    return jnp.minimum(jnp.maximum(result, -most), most).astype(kind)


def setup_inputs(seed: int = 0) -> dict:
    streams_of = jax.random.split(jax.random.key(seed), 7)
    data_real = scatter_about(streams_of[0], (F, N, N), (N // 4) ** -0.5, 0.5, ((0, 4), (1, 8)))
    data_imaginary = scatter_about(streams_of[1], (F, N, N), (N // 4) ** -0.5, 0.5, ((0, 4), (1, 8)))
    wavelet_real = scatter_about(streams_of[2], (F,), 0.7, 2.5, ((0, 4),), jnp.float32)
    wavelet_imaginary = scatter_about(streams_of[3], (F,), 0.7, 2.5, ((0, 4),), jnp.float32)
    primaries_real = scatter_about(streams_of[4], (F, N, N), 0.5, 3.0, ((0, 4), (1, 8)), jnp.float32)
    primaries_imaginary = scatter_about(streams_of[5], (F, N, N), 0.5, 3.0, ((0, 4), (1, 8)), jnp.float32)
    return dict(data_real=data_real, data_imaginary=data_imaginary, wavelet_real=wavelet_real, wavelet_imaginary=wavelet_imaginary, primaries_real=primaries_real, primaries_imaginary=primaries_imaginary)


STEP_LENGTH = 0.02
THRESHOLD = 0.25


def forward_product(left, right):
    return jnp.einsum("frk,fkc->frc", left, right, precision=lax.Precision.HIGHEST)


def adjoint_product(left, right):
    return jnp.einsum("frk,fjk->frj", left, right, precision=lax.Precision.HIGHEST)


def rounded(values):
    return lax.optimization_barrier(values.astype(jnp.bfloat16)).astype(jnp.float32)


def reference(data_real, data_imaginary, wavelet_real, wavelet_imaginary, primaries_real, primaries_imaginary):
    slab_real = data_real.astype(jnp.float32)
    slab_imaginary = data_imaginary.astype(jnp.float32)
    wave_real = wavelet_real[:, None, None]
    wave_imaginary = wavelet_imaginary[:, None, None]
    current_real = primaries_real
    current_imaginary = primaries_imaginary
    misfits = []
    for iteration in range(ITERS):
        rounded_real = rounded(current_real)
        rounded_imaginary = rounded(current_imaginary)
        forward_real = forward_product(rounded_real, slab_real) - forward_product(rounded_imaginary, slab_imaginary)
        forward_imaginary = forward_product(rounded_real, slab_imaginary) + forward_product(rounded_imaginary, slab_real)
        error_real = slab_real + forward_real - (wave_real * current_real - wave_imaginary * current_imaginary)
        error_imaginary = slab_imaginary + forward_imaginary - (wave_real * current_imaginary + wave_imaginary * current_real)
        total = jnp.sum(error_real * error_real) + jnp.sum(error_imaginary * error_imaginary)
        misfits.append(total / (F * N * N))
        eb_real = rounded(error_real)
        eb_imaginary = rounded(error_imaginary)
        back_real = adjoint_product(eb_real, slab_real) + adjoint_product(eb_imaginary, slab_imaginary)
        back_imaginary = adjoint_product(eb_imaginary, slab_real) - adjoint_product(eb_real, slab_imaginary)
        gradient_real = wave_real * error_real + wave_imaginary * error_imaginary - back_real
        gradient_imaginary = wave_real * error_imaginary - wave_imaginary * error_real - back_imaginary
        stepped_real = current_real + STEP_LENGTH * gradient_real
        stepped_imaginary = current_imaginary + STEP_LENGTH * gradient_imaginary
        in_time = jnp.fft.ifft(stepped_real + 1j * stepped_imaginary, axis=0, norm="ortho")
        time_real = jnp.real(in_time)
        time_imaginary = jnp.imag(in_time)
        shrunk_real = time_real - jnp.clip(time_real, -THRESHOLD, THRESHOLD)
        shrunk_imaginary = time_imaginary - jnp.clip(time_imaginary, -THRESHOLD, THRESHOLD)
        in_frequency = jnp.fft.fft(shrunk_real + 1j * shrunk_imaginary, axis=0, norm="ortho")
        current_real = jnp.real(in_frequency).astype(jnp.float32)
        current_imaginary = jnp.imag(in_frequency).astype(jnp.float32)
    return current_real, current_imaginary, jnp.stack(misfits).astype(jnp.float32)
```

```python
import functools
import math

import jax
import jax.numpy as jnp
from jax import lax
from jax.experimental import pallas as pl
from jax.experimental.pallas import tpu as pltpu
from jax.sharding import PartitionSpec as P

ITERS = 2
STEP_LENGTH = 0.02
THRESHOLD = 0.25
CHUNKS = 4
GROUP = 8
HALF = math.sqrt(0.5)
MESH = pl.DeviceIdType.MESH


def product_kernel(first, offset, wr_ref, wi_ref, whole_ref, own_r_ref, own_i_ref, *rest):
    if first:
        gr_ref, gi_ref, out_ref, sum_ref = rest
        gr = gr_ref[0]
        gi = gi_ref[0]
    else:
        g_ref, out_ref, sum_ref = rest
        parts = g_ref.shape[0]
        gr = jnp.concatenate([g_ref[a, 0, 0] for a in range(parts)], axis=1)
        gi = jnp.concatenate([g_ref[a, 1, 0] for a in range(parts)], axis=1)
    at = pl.program_id(0) + offset
    qr = wr_ref[at]
    qi = wi_ref[at]
    rows = gr.shape[0]
    n = gr.shape[1]
    whole_r = whole_ref[:, 0, 0].reshape(n, n)
    whole_i = whole_ref[:, 1, 0].reshape(n, n)
    left = jnp.concatenate([gr.astype(jnp.bfloat16), gi.astype(jnp.bfloat16)], axis=0)
    pr = jnp.dot(left, whole_r, preferred_element_type=jnp.float32)
    pi = jnp.dot(left, whole_i, preferred_element_type=jnp.float32)
    er = own_r_ref[0].astype(jnp.float32) + (pr[:rows] - pi[rows:]) - (qr * gr - qi * gi)
    ei = own_i_ref[0].astype(jnp.float32) + (pi[:rows] + pr[rows:]) - (qr * gi + qi * gr)
    sum_ref[0] = jnp.sum(er * er + ei * ei, axis=0, keepdims=True)
    eb = jnp.concatenate([er.astype(jnp.bfloat16), ei.astype(jnp.bfloat16)], axis=0)
    dims = (((1,), (1,)), ((), ()))
    br = lax.dot_general(eb, whole_r, dims, preferred_element_type=jnp.float32)
    bi = lax.dot_general(eb, whole_i, dims, preferred_element_type=jnp.float32)
    hr = qr * er + qi * ei - (br[:rows] + bi[rows:])
    hi = qr * ei - qi * er - (br[rows:] - bi[:rows])
    zr = gr + STEP_LENGTH * hr
    zi = gi + STEP_LENGTH * hi
    parts = out_ref.shape[0]
    width = n // parts
    for a in range(parts):
        out_ref[a, 0, 0] = zr[:, a * width : (a + 1) * width]
        out_ref[a, 1, 0] = zi[:, a * width : (a + 1) * width]


def product(offset, count, parts, wr, wi, whole, own_r, own_i, current):
    sa, _, _, rows, n = whole.shape
    first = len(current) == 2
    plain = pl.BlockSpec((1, rows, n), lambda f: (f + offset, 0, 0))
    scalars = pl.BlockSpec(memory_space=pltpu.SMEM)
    width = n // parts
    if first:
        cur_specs = [plain, plain]
    else:
        cur_specs = [pl.BlockSpec((parts, 2, 1, rows, width), lambda f: (0, 0, f + offset, 0, 0))]
    return pl.pallas_call(
        functools.partial(product_kernel, first, offset),
        grid=(count,),
        in_specs=[scalars, scalars, pl.BlockSpec((sa, 2, 1, rows, n), lambda f: (0, 0, f, 0, 0)), plain, plain]
        + cur_specs,
        out_specs=[
            pl.BlockSpec((parts, 2, 1, rows, width), lambda f: (0, 0, f, 0, 0)),
            pl.BlockSpec((1, 1, n), lambda f: (f, 0, 0)),
        ],
        out_shape=[
            jax.ShapeDtypeStruct((parts, 2, count, rows, width), jnp.float32),
            jax.ShapeDtypeStruct((count, 1, n), jnp.float32),
        ],
        cost_estimate=pl.CostEstimate(
            flops=16 * count * rows * n * n, bytes_accessed=count * n * (n * 4 + rows * 20), transcendentals=0
        ),
        compiler_params=pltpu.CompilerParams(vmem_limit_bytes=60 * 2**20),
    )(wr, wi, whole, own_r, own_i, *current)


def add(a, b):
    return (a[0] + b[0], a[1] + b[1])


def sub(a, b):
    return (a[0] - b[0], a[1] - b[1])


def turn(a, sign):
    return (-a[1], a[0]) if sign > 0 else (a[1], -a[0])


def rotate(a, turns):
    c, s = math.cos(2 * math.pi * turns), math.sin(2 * math.pi * turns)
    return (a[0] * c - a[1] * s, a[0] * s + a[1] * c)


def four(a, b, c, d, sign):
    s0, s1, s2, s3 = add(a, c), sub(a, c), add(b, d), turn(sub(b, d), sign)
    return add(s0, s2), add(s1, s3), sub(s0, s2), sub(s1, s3)


def eight(x, sign):
    even = four(x[0], x[2], x[4], x[6], sign)
    odd = four(x[1], x[3], x[5], x[7], sign)
    o1 = add(odd[1], turn(odd[1], sign))
    o3 = sub(turn(odd[3], sign), odd[3])
    odd = (odd[0], (o1[0] * HALF, o1[1] * HALF), turn(odd[2], sign), (o3[0] * HALF, o3[1] * HALF))
    return [add(even[k], odd[k]) for k in range(4)] + [sub(even[k], odd[k]) for k in range(4)]


def shrink(v):
    return v - jnp.clip(v, -THRESHOLD, THRESHOLD)


def transform_kernel(pieces, in_scale, out_scale, *refs):
    in_refs, out_ref, work = refs[:pieces], refs[pieces], refs[pieces + 1]
    parts, _, local, block, width = out_ref.shape
    piece = local // pieces
    radix = 8
    factor = 1.0 / radix

    def one(g, _):
        at = pl.ds(pl.multiple_of(g * GROUP, GROUP), GROUP)

        def load(f):
            a, b = divmod(f, local)
            c, d = divmod(b, piece)
            ref = in_refs[c]
            scale = factor * in_scale
            return (
                ref[a, 0, d, at, :].astype(jnp.float32) * scale,
                ref[a, 1, d, at, :].astype(jnp.float32) * scale,
            )

        for f1 in range(radix):
            y = eight([load(f1 + radix * f2) for f2 in range(radix)], 1)
            for t2 in range(radix):
                v = rotate(y[t2], f1 * t2 / 64) if f1 * t2 else y[t2]
                work[0, radix * f1 + t2] = v[0]
                work[1, radix * f1 + t2] = v[1]
        for t2 in range(radix):
            y = eight([(work[0, radix * f1 + t2], work[1, radix * f1 + t2]) for f1 in range(radix)], 1)
            y = [(shrink(v[0]), shrink(v[1])) for v in y]
            y = eight(y, -1)
            for f1 in range(radix):
                v = rotate(y[f1], -f1 * t2 / 64) if f1 * t2 else y[f1]
                work[0, radix * f1 + t2] = v[0]
                work[1, radix * f1 + t2] = v[1]
        for f1 in range(radix):
            y = eight([(work[0, radix * f1 + t2], work[1, radix * f1 + t2]) for t2 in range(radix)], -1)
            for f2 in range(radix):
                a, b = divmod(f1 + radix * f2, local)
                scale = factor * out_scale
                out_ref[a, 0, b, at, :] = y[f2][0] * scale
                out_ref[a, 1, b, at, :] = y[f2][1] * scale
        return 0

    lax.fori_loop(0, block // GROUP, one, 0)


def transform(arrays, in_scale, out_scale):
    pieces = len(arrays)
    parts, _, piece, rows, width = arrays[0].shape
    local = piece * pieces
    block = min(16, rows)
    return pl.pallas_call(
        functools.partial(transform_kernel, pieces, in_scale, out_scale),
        grid=(rows // block,),
        in_specs=[pl.BlockSpec((parts, 2, piece, block, width), lambda r: (0, 0, 0, r, 0))] * pieces,
        out_specs=pl.BlockSpec((parts, 2, local, block, width), lambda r: (0, 0, 0, r, 0)),
        out_shape=jax.ShapeDtypeStruct((parts, 2, local, rows, width), jnp.float32),
        scratch_shapes=[pltpu.VMEM((2, parts * local, GROUP, width), jnp.float32)],
        cost_estimate=pl.CostEstimate(
            flops=4000 * rows * width, bytes_accessed=16 * parts * local * rows * width, transcendentals=0
        ),
        compiler_params=pltpu.CompilerParams(vmem_limit_bytes=60 * 2**20),
    )(*arrays)


def total_kernel(counts, own_ref, out_ref, slots, send_sem, recv_sem):
    afs, sas = counts
    n = afs * sas
    me = lax.axis_index("af") * sas + lax.axis_index("sa")

    def peer(k):
        p = lax.rem(me + k, n)
        return (p // sas, lax.rem(p, sas))

    def hello(k, _):
        pl.semaphore_signal(barrier, inc=1, device_id=peer(k), device_id_type=MESH)
        return 0

    def copy(k):
        return pltpu.make_async_remote_copy(
            src_ref=own_ref,
            dst_ref=slots.at[k],
            send_sem=send_sem.at[k],
            recv_sem=recv_sem.at[k],
            device_id=peer(k),
            device_id_type=MESH,
        )

    def start(k, _):
        copy(k).start()
        return 0

    def finish(k, value):
        copy(k).wait()
        return value + slots[k]

    barrier = pltpu.get_barrier_semaphore()
    lax.fori_loop(1, n, hello, 0)
    pl.semaphore_wait(barrier, n - 1)
    lax.fori_loop(1, n, start, 0)
    out_ref[...] = lax.fori_loop(1, n, finish, own_ref[...])


def total(own, counts):
    n = counts[0] * counts[1]
    return pl.pallas_call(
        functools.partial(total_kernel, counts),
        out_shape=jax.ShapeDtypeStruct(own.shape, own.dtype),
        in_specs=[pl.BlockSpec(memory_space=pltpu.VMEM)],
        out_specs=pl.BlockSpec(memory_space=pltpu.VMEM),
        scratch_shapes=[
            pltpu.VMEM((n, *own.shape), own.dtype),
            pltpu.SemaphoreType.DMA((n,)),
            pltpu.SemaphoreType.DMA((n,)),
        ],
        compiler_params=pltpu.CompilerParams(collective_id=0, has_side_effects=True),
    )(own)


def exchange(values):
    return lax.all_to_all(values, "af", split_axis=0, concat_axis=0, tiled=True)


def on_device(counts, data_real, data_imaginary, wave_real, wave_imaginary, primaries_real, primaries_imaginary):
    parts = counts[0]
    local, rows, n = data_real.shape
    size = local // CHUNKS
    wholes = []
    for c in range(CHUNKS):
        cut = slice(c * size, (c + 1) * size)
        both = jnp.stack([data_real[cut], data_imaginary[cut]])
        wholes.append(lax.all_gather(both, "sa", axis=0))
    first = (primaries_real, primaries_imaginary)
    sums = []
    current = None
    for iteration in range(ITERS):
        wire = jnp.float16 if iteration == 0 else jnp.float32
        traces = []
        squares = []
        for c in range(CHUNKS):
            stepped, square = product(
                c * size, size, parts, wave_real, wave_imaginary, wholes[c], data_real, data_imaginary,
                first if iteration == 0 else (current,),
            )
            squares.append(square)
            traces.append(exchange(stepped.astype(wire)).astype(jnp.float32))
        sums.append(jnp.sum(jnp.concatenate(squares)))
        scale = 0.25 if iteration == 0 else 1.0
        back = transform(traces, 1.0, scale)
        current = exchange(back.astype(wire)).astype(jnp.float32)
        if iteration == 0:
            current = current / scale
    updated = current.transpose(1, 2, 3, 0, 4).reshape(2, local, rows, n)
    row = lax.broadcasted_iota(jnp.int32, (8, 128), 0)
    own = jnp.where(row == 0, sums[0], jnp.where(row == 1, sums[1], 0.0))
    misfit = total(own, counts)[:ITERS, 0] / (parts * local * n * n)
    return (updated[0], updated[1], misfit)


def solution(mesh):
    split = P("af", "sa", None)
    counts = (mesh.shape["af"], mesh.shape["sa"])
    return jax.shard_map(
        functools.partial(on_device, counts),
        mesh=mesh,
        in_specs=(split, split, P("af"), P("af"), split, split),
        out_specs=(split, split, P()),
        check_vma=False,
    )
```

```python
import functools
import math

import jax
import jax.numpy as jnp
from jax import lax
from jax.experimental import pallas as pl
from jax.experimental.pallas import tpu as pltpu
from jax.sharding import PartitionSpec as P

ITERS = 2
STEP_LENGTH = 0.02
THRESHOLD = 0.25
CHUNKS = 2
WIRE = jnp.float16
LARGEST = 60000.0
GROUP = 8
HALF = math.sqrt(0.5)
MESH = pl.DeviceIdType.MESH


def product_kernel(first, offset, wr_ref, wi_ref, whole_ref, own_r_ref, own_i_ref, *rest):
    if first:
        gr_ref, gi_ref, out_ref, sum_ref = rest
        gr = gr_ref[0]
        gi = gi_ref[0]
    else:
        g_ref, gi_ref, out_ref, sum_ref = rest
        parts = g_ref.shape[0]
        gr = jnp.concatenate([g_ref[a, 0] for a in range(parts)], axis=1)
        gi = jnp.concatenate([gi_ref[a, 0] for a in range(parts)], axis=1)
    at = pl.program_id(0) + offset
    qr = wr_ref[at]
    qi = wi_ref[at]
    rows = gr.shape[0]
    n = gr.shape[1]
    whole_r = whole_ref[:, 0, 0].reshape(n, n)
    whole_i = whole_ref[:, 1, 0].reshape(n, n)
    left = jnp.concatenate([gr.astype(jnp.bfloat16), gi.astype(jnp.bfloat16)], axis=0)
    pr = jnp.dot(left, whole_r, preferred_element_type=jnp.float32)
    pi = jnp.dot(left, whole_i, preferred_element_type=jnp.float32)
    er = own_r_ref[0].astype(jnp.float32) + (pr[:rows] - pi[rows:]) - (qr * gr - qi * gi)
    ei = own_i_ref[0].astype(jnp.float32) + (pi[:rows] + pr[rows:]) - (qr * gi + qi * gr)
    sum_ref[0] = jnp.sum(er * er + ei * ei, axis=0, keepdims=True)
    eb = jnp.concatenate([er.astype(jnp.bfloat16), ei.astype(jnp.bfloat16)], axis=0)
    dims = (((1,), (1,)), ((), ()))
    br = lax.dot_general(eb, whole_r, dims, preferred_element_type=jnp.float32)
    bi = lax.dot_general(eb, whole_i, dims, preferred_element_type=jnp.float32)
    hr = qr * er + qi * ei - (br[:rows] + bi[rows:])
    hi = qr * ei - qi * er - (br[rows:] - bi[:rows])
    zr = gr + STEP_LENGTH * hr
    zi = gi + STEP_LENGTH * hi
    parts = out_ref.shape[0]
    width = n // parts
    for a in range(parts):
        out_ref[a, 0, 0] = zr[:, a * width : (a + 1) * width]
        out_ref[a, 1, 0] = zi[:, a * width : (a + 1) * width]


def product(offset, count, local, parts, wr, wi, whole, own_r, own_i, current):
    sa, _, _, rows, n = whole.shape
    first = len(current) == 2
    plain = pl.BlockSpec((1, rows, n), lambda f: (f + offset, 0, 0))
    scalars = pl.BlockSpec(memory_space=pltpu.SMEM)
    width = n // parts
    if first:
        cur_specs = [plain, plain]
    else:
        block = (parts, 1, rows, width)
        cur_specs = [
            pl.BlockSpec(block, lambda f: (0, f + offset, 0, 0)),
            pl.BlockSpec(block, lambda f: (0, f + offset + local, 0, 0)),
        ]
        current = (current[0], current[0])
    return pl.pallas_call(
        functools.partial(product_kernel, first, offset),
        grid=(count,),
        in_specs=[scalars, scalars, pl.BlockSpec((sa, 2, 1, rows, n), lambda f: (0, 0, f, 0, 0)), plain, plain]
        + cur_specs,
        out_specs=[
            pl.BlockSpec((parts, 2, 1, rows, width), lambda f: (0, 0, f, 0, 0)),
            pl.BlockSpec((1, 1, n), lambda f: (f, 0, 0)),
        ],
        out_shape=[
            jax.ShapeDtypeStruct((parts, 2, count, rows, width), jnp.float32),
            jax.ShapeDtypeStruct((count, 1, n), jnp.float32),
        ],
        cost_estimate=pl.CostEstimate(
            flops=16 * count * rows * n * n, bytes_accessed=count * n * (n * 4 + rows * 20), transcendentals=0
        ),
        compiler_params=pltpu.CompilerParams(vmem_limit_bytes=60 * 2**20),
    )(wr, wi, whole, own_r, own_i, *current)


def add(a, b):
    return (a[0] + b[0], a[1] + b[1])


def sub(a, b):
    return (a[0] - b[0], a[1] - b[1])


def turn(a, sign):
    return (-a[1], a[0]) if sign > 0 else (a[1], -a[0])


def rotate(a, turns):
    c, s = math.cos(2 * math.pi * turns), math.sin(2 * math.pi * turns)
    return (a[0] * c - a[1] * s, a[0] * s + a[1] * c)


def four(a, b, c, d, sign):
    s0, s1, s2, s3 = add(a, c), sub(a, c), add(b, d), turn(sub(b, d), sign)
    return add(s0, s2), add(s1, s3), sub(s0, s2), sub(s1, s3)


def eight(x, sign):
    even = four(x[0], x[2], x[4], x[6], sign)
    odd = four(x[1], x[3], x[5], x[7], sign)
    o1 = add(odd[1], turn(odd[1], sign))
    o3 = sub(turn(odd[3], sign), odd[3])
    odd = (odd[0], (o1[0] * HALF, o1[1] * HALF), turn(odd[2], sign), (o3[0] * HALF, o3[1] * HALF))
    return [add(even[k], odd[k]) for k in range(4)] + [sub(even[k], odd[k]) for k in range(4)]


def shrink(v):
    return v - jnp.clip(v, -THRESHOLD, THRESHOLD)


def transform_kernel(pieces, bound, *refs):
    scale_ref, in_refs, out_ref, work = refs[0], refs[1 : pieces + 1], refs[pieces + 1], refs[pieces + 2]
    parts, slots, block, width = out_ref.shape
    local = slots // 2
    piece = local // pieces
    radix = 8
    in_scale = scale_ref[0] / radix
    out_scale = scale_ref[1] / radix

    def one(g, _):
        at = pl.ds(pl.multiple_of(g * GROUP, GROUP), GROUP)

        def load(f):
            a, b = divmod(f, local)
            c, d = divmod(b, piece)
            ref = in_refs[c]
            return (
                ref[a, 0, d, at, :].astype(jnp.float32) * in_scale,
                ref[a, 1, d, at, :].astype(jnp.float32) * in_scale,
            )

        for f1 in range(radix):
            y = eight([load(f1 + radix * f2) for f2 in range(radix)], 1)
            for t2 in range(radix):
                v = rotate(y[t2], f1 * t2 / 64) if f1 * t2 else y[t2]
                work[0, radix * f1 + t2] = v[0]
                work[1, radix * f1 + t2] = v[1]
        for t2 in range(radix):
            y = eight([(work[0, radix * f1 + t2], work[1, radix * f1 + t2]) for f1 in range(radix)], 1)
            y = [(shrink(v[0]), shrink(v[1])) for v in y]
            y = eight(y, -1)
            for f1 in range(radix):
                v = rotate(y[f1], -f1 * t2 / 64) if f1 * t2 else y[f1]
                work[0, radix * f1 + t2] = v[0]
                work[1, radix * f1 + t2] = v[1]
        largest = jnp.zeros((GROUP, width), jnp.float32)
        for f1 in range(radix):
            y = eight([(work[0, radix * f1 + t2], work[1, radix * f1 + t2]) for t2 in range(radix)], -1)
            for f2 in range(radix):
                a, b = divmod(f1 + radix * f2, local)
                re, im = y[f2][0] * out_scale, y[f2][1] * out_scale
                out_ref[a, b, at, :] = re
                out_ref[a, b + local, at, :] = im
                if bound:
                    largest = jnp.maximum(largest, jnp.maximum(jnp.abs(re), jnp.abs(im)))
        if bound:
            for a in range(parts):
                out_ref[a, 2 * local, at, :] = largest
        return 0

    lax.fori_loop(0, block // GROUP, one, 0)


def transform(arrays, in_scale, out_scale, bound):
    pieces = len(arrays)
    parts, _, piece, rows, width = arrays[0].shape
    local = piece * pieces
    block = min(16, rows)
    slots = 2 * local + (1 if bound else 0)
    scales = jnp.stack([jnp.float32(in_scale), jnp.float32(out_scale)])
    return pl.pallas_call(
        functools.partial(transform_kernel, pieces, bound),
        grid=(rows // block,),
        in_specs=[pl.BlockSpec(memory_space=pltpu.SMEM)]
        + [pl.BlockSpec((parts, 2, piece, block, width), lambda r: (0, 0, 0, r, 0))] * pieces,
        out_specs=pl.BlockSpec((parts, slots, block, width), lambda r: (0, 0, r, 0)),
        out_shape=jax.ShapeDtypeStruct((parts, slots, rows, width), jnp.float32),
        scratch_shapes=[pltpu.VMEM((2, parts * local, GROUP, width), jnp.float32)],
        cost_estimate=pl.CostEstimate(
            flops=4000 * rows * width, bytes_accessed=16 * parts * local * rows * width, transcendentals=0
        ),
        compiler_params=pltpu.CompilerParams(vmem_limit_bytes=60 * 2**20),
    )(scales, *arrays)


def total_kernel(counts, own_ref, out_ref, slots, send_sem, recv_sem):
    afs, sas = counts
    n = afs * sas
    me = lax.axis_index("af") * sas + lax.axis_index("sa")

    def peer(k):
        p = lax.rem(me + k, n)
        return (p // sas, lax.rem(p, sas))

    def hello(k, _):
        pl.semaphore_signal(barrier, inc=1, device_id=peer(k), device_id_type=MESH)
        return 0

    def copy(k):
        return pltpu.make_async_remote_copy(
            src_ref=own_ref,
            dst_ref=slots.at[k],
            send_sem=send_sem.at[k],
            recv_sem=recv_sem.at[k],
            device_id=peer(k),
            device_id_type=MESH,
        )

    def start(k, _):
        copy(k).start()
        return 0

    def finish(k, value):
        copy(k).wait()
        return value + slots[k]

    barrier = pltpu.get_barrier_semaphore()
    lax.fori_loop(1, n, hello, 0)
    pl.semaphore_wait(barrier, n - 1)
    lax.fori_loop(1, n, start, 0)
    out_ref[...] = lax.fori_loop(1, n, finish, own_ref[...])


def total(own, counts):
    n = counts[0] * counts[1]
    return pl.pallas_call(
        functools.partial(total_kernel, counts),
        out_shape=jax.ShapeDtypeStruct(own.shape, own.dtype),
        in_specs=[pl.BlockSpec(memory_space=pltpu.VMEM)],
        out_specs=pl.BlockSpec(memory_space=pltpu.VMEM),
        scratch_shapes=[
            pltpu.VMEM((n, *own.shape), own.dtype),
            pltpu.SemaphoreType.DMA((n,)),
            pltpu.SemaphoreType.DMA((n,)),
        ],
        compiler_params=pltpu.CompilerParams(collective_id=0, has_side_effects=True),
    )(own)


def exchange(values):
    return lax.all_to_all(values, "af", split_axis=0, concat_axis=0, tiled=True)


def join_kernel(scale_ref, re_ref, im_ref, out_re, out_im):
    parts, _, _, width = re_ref.shape
    scale = scale_ref[0]
    for a in range(parts):
        cut = slice(a * width, (a + 1) * width)
        out_re[:, :, cut] = re_ref[a] * scale
        out_im[:, :, cut] = im_ref[a] * scale


def join(current, scale, local):
    parts, _, rows, width = current.shape
    count = max(1, local // 4)
    out = jax.ShapeDtypeStruct((local, rows, parts * width), jnp.float32)
    out_spec = pl.BlockSpec((count, rows, parts * width), lambda f: (f, 0, 0))
    block = (parts, count, rows, width)
    steps = local // count
    return pl.pallas_call(
        join_kernel,
        grid=(steps,),
        in_specs=[
            pl.BlockSpec(memory_space=pltpu.SMEM),
            pl.BlockSpec(block, lambda f: (0, f, 0, 0)),
            pl.BlockSpec(block, lambda f: (0, f + steps, 0, 0)),
        ],
        out_specs=[out_spec, out_spec],
        out_shape=[out, out],
        compiler_params=pltpu.CompilerParams(vmem_limit_bytes=60 * 2**20),
    )(scale.reshape(1), current, current)


def on_device(counts, data_real, data_imaginary, wave_real, wave_imaginary, primaries_real, primaries_imaginary):
    parts = counts[0]
    local, rows, n = data_real.shape
    freqs = local * parts
    size = local // CHUNKS
    wholes = []
    for c in range(CHUNKS):
        cut = slice(c * size, (c + 1) * size)
        both = jnp.stack([data_real[cut], data_imaginary[cut]])
        wholes.append(lax.all_gather(both, "sa", axis=0))
    gain = 1.01 * (2 * 2.5 + n)
    spread = 1.01 * math.sqrt(2 * freqs)

    def stepped_bound(g):
        return g + STEP_LENGTH * gain * (0.5 + gain * g)

    z_scale = 1.0
    z_bound = stepped_bound(3.0)
    sums = []
    current = (primaries_real, primaries_imaginary)
    for iteration in range(ITERS):
        last = iteration == ITERS - 1
        traces = [None] * CHUNKS
        squares = []
        for c in range(CHUNKS):
            stepped, square = product(
                c * size, size, local, parts, wave_real, wave_imaginary, wholes[c], data_real, data_imaginary, current,
            )
            squares.append(square)
            traces[c] = exchange((stepped * (1.0 / z_scale)).astype(WIRE)).astype(jnp.float32)
        sums.append(jnp.sum(jnp.concatenate(squares)))
        g_scale = spread * z_bound / LARGEST
        back = transform(traces, z_scale, 1.0 / g_scale, not last)
        moved = exchange(back.astype(WIRE)).astype(jnp.float32)
        if last:
            updated = join(moved, jnp.float32(g_scale), local)
        else:
            g_bound = 1.002 * g_scale * jnp.max(moved[:, 2 * local]) + 1e-6
            current = (moved * g_scale,)
            z_bound = stepped_bound(g_bound)
            z_scale = z_bound / LARGEST
    row = lax.broadcasted_iota(jnp.int32, (8, 128), 0)
    own = jnp.where(row == 0, sums[0], jnp.where(row == 1, sums[1], 0.0))
    misfit = total(own, counts)[:ITERS, 0] / (freqs * n * n)
    return (updated[0], updated[1], misfit)


def solution(mesh):
    split = P("af", "sa", None)
    counts = (mesh.shape["af"], mesh.shape["sa"])
    return jax.shard_map(
        functools.partial(on_device, counts),
        mesh=mesh,
        in_specs=(split, split, P("af"), P("af"), split, split),
        out_specs=(split, split, P()),
        check_vma=False,
    )
```
